256 devices in a mesh: row: 8 (over y, z_hi), col: 32 (over x, z_lo, core).
Axes of the slice: x: 4, y: 4, z: 8 (z_hi: 2, z_lo: 4; z = z_hi * 4 + z_lo), core: 2. Of those that a mesh axis runs over, the one named last changes fastest.
Arguments:
- previous: bfloat16 [4, 128, 256, 256], P(None, 'row', 'col'), may hold values from -6 to 6
- skip_coarse: bfloat16 [4, 128, 256, 256], P(None, 'row', 'col'), may hold values from -6 to 6
- skip_fine: bfloat16 [4, 256, 512, 256], P(None, 'row', 'col'), may hold values from -6 to 6
- coarse_convs: bfloat16 [4, 3, 3, 256, 256], replicated, may hold values from -0.125 to 0.125
- coarse_biases: float32 [4, 256], replicated, may hold values from -3 to 3
- coarse_project: bfloat16 [256, 256], replicated, may hold values from -0.375 to 0.375
- coarse_offset: float32 [256], replicated, may hold values from -3 to 3
- fine_convs: bfloat16 [4, 3, 3, 256, 256], replicated, may hold values from -0.125 to 0.125
- fine_biases: float32 [4, 256], replicated, may hold values from -3 to 3
- fine_project: bfloat16 [256, 256], replicated, may hold values from -0.375 to 0.375
- fine_offset: float32 [256], replicated, may hold values from -3 to 3
Outputs:
- decoded: bfloat16 [4, 512, 1024, 256], P(None, 'row', 'col')
The draws below stay inside these ranges and needn't reach their ends.
All inputs are finite; a program needn't handle non-finite values.
Results may differ from the reference program's by a relative error of at most 0.012.
Values may be sent and summed in bfloat16 or wider, within the bound.
A program may use at most 128 MiB of HBM per device.

```python
import jax
import jax.numpy as jnp
from jax import lax

C = 256
B = 4
H8 = 128
W8 = 256


def level_of(key, shape, cuts, low, high):
    def one(axis_at, parts):
        draws = jax.random.uniform(jax.random.fold_in(jax.random.fold_in(key, 6), axis_at), (parts,), jnp.float32, low / len(cuts), high / len(cuts))
        return jnp.repeat(jnp.exp(draws), shape[axis_at] // parts).reshape((-1,) + (1,) * (len(shape) - axis_at - 1))

    loudness = one(*cuts[0])
    for cut in cuts[1:]:
        loudness = loudness * one(*cut)
    return loudness


def centred(key, shape, spread, most, shards=(), dtype=jnp.bfloat16):
    drawn = jax.random.normal(key, shape, jnp.float32) * spread
    if len(shards) > 0:
        drawn = level_of(key, shape, shards, -0.22, 0.18) * drawn
    return jnp.clip(drawn, min=-most, max=most).astype(dtype)


def setup_inputs(seed: int = 0) -> dict:
    key_list = jax.random.split(jax.random.key(seed), 12)
    return {
        "previous": centred(key_list[0], (B, H8, W8, C), 1.0, 6.0, ((1, 8), (2, 32))),
        "skip_coarse": centred(key_list[1], (B, H8, W8, C), 1.0, 6.0, ((1, 8), (2, 32))),
        "skip_fine": centred(key_list[2], (B, 2 * H8, 2 * W8, C), 1.0, 6.0, ((1, 8), (2, 32))),
        "coarse_convs": centred(key_list[3], (4, 3, 3, C, C), (9 * C) ** -0.5, 0.125),
        "coarse_biases": centred(key_list[4], (4, C), 0.5, 3.0, (), jnp.float32),
        "coarse_project": centred(key_list[5], (C, C), C ** -0.5, 0.375),
        "coarse_offset": centred(key_list[6], (C,), 0.5, 3.0, (), jnp.float32),
        "fine_convs": centred(key_list[7], (4, 3, 3, C, C), (9 * C) ** -0.5, 0.125),
        "fine_biases": centred(key_list[8], (4, C), 0.5, 3.0, (), jnp.float32),
        "fine_project": centred(key_list[9], (C, C), C ** -0.5, 0.375),
        "fine_offset": centred(key_list[10], (C,), 0.5, 3.0, (), jnp.float32),
    }


def convolve(image, kernel, bias):
    padded = jnp.pad(image, ((0, 0), (1, 1), (1, 1), (0, 0)))
    result = lax.conv_general_dilated(padded, kernel, (1, 1), "VALID", dimension_numbers=("NHWC", "HWIO", "NHWC"), preferred_element_type=jnp.float32)
    return result + bias


def residual_unit(inputs, kernels, biases, first):
    active = jax.nn.relu(inputs).astype(jnp.bfloat16)
    hidden = jax.nn.relu(convolve(active, kernels[first], biases[first])).astype(jnp.bfloat16)
    return inputs.astype(jnp.float32) + convolve(hidden, kernels[first + 1], biases[first + 1])


def double_axis(values, axis):
    count = values.shape[axis]
    padded = jnp.concatenate([lax.slice_in_dim(values, 0, 1, axis=axis), values, lax.slice_in_dim(values, count - 1, count, axis=axis)], axis=axis)
    before = lax.slice_in_dim(padded, 0, count, axis=axis)
    after = lax.slice_in_dim(padded, 2, count + 2, axis=axis)
    even = 0.75 * values + 0.25 * before
    odd = 0.75 * values + 0.25 * after
    stacked = jnp.stack([even, odd], axis=axis + 1)
    shape = list(values.shape)
    shape[axis] = 2 * count
    return stacked.reshape(shape)


def upsample(image):
    values = image.astype(jnp.float32)
    return double_axis(double_axis(values, 1), 2).astype(jnp.bfloat16)


def reference(previous, skip_coarse, skip_fine, coarse_convs, coarse_biases, coarse_project, coarse_offset, fine_convs, fine_biases, fine_project, fine_offset):
    sum_coarse = previous.astype(jnp.float32) + residual_unit(skip_coarse, coarse_convs, coarse_biases, 0)
    top_coarse = residual_unit(sum_coarse, coarse_convs, coarse_biases, 2).astype(jnp.bfloat16)
    joined_coarse = (jnp.dot(upsample(top_coarse), coarse_project, preferred_element_type=jnp.float32) + coarse_offset).astype(jnp.bfloat16)
    sum_fine = joined_coarse.astype(jnp.float32) + residual_unit(skip_fine, fine_convs, fine_biases, 0)
    top_fine = residual_unit(sum_fine, fine_convs, fine_biases, 2).astype(jnp.bfloat16)
    return (jnp.dot(upsample(top_fine), fine_project, preferred_element_type=jnp.float32) + fine_offset).astype(jnp.bfloat16)
```

```python
import functools

import jax
import jax.numpy as jnp
import numpy as np
from jax import lax
from jax.experimental import pallas as pl
from jax.experimental.pallas import tpu as pltpu
from jax.sharding import PartitionSpec as P

MESH = pl.DeviceIdType.MESH
F32 = jnp.float32
BF16 = jnp.bfloat16
C = 256
B = 4
HC, WC = 16, 8
HF, WF = 32, 16
DIRS = ((-1, 0), (1, 0), (0, -1), (0, 1), (-1, -1), (1, 1), (-1, 1), (1, -1))


class Halo:
    def __init__(self, height, width, rows, cols):
        self.h, self.w, self.mr, self.mc = height, width, rows, cols
        self.off = B * cols
        sizes = [rows * B * width] * 2 + [height * B * cols] * 2 + [rows * B * cols] * 4
        self.sizes = sizes
        self.starts = [sum(sizes[:d]) for d in range(8)]
        self.total = sum(sizes)

    def part(self, d):
        return pl.ds(self.starts[d], self.sizes[d])

    def span(self, step, edge, length, margin):
        if step == 0:
            return margin, length
        if step < 0:
            return (margin if edge else 0), margin
        return (length if edge else margin + length), margin

    def box(self, d, edge):
        r0, rn = self.span(DIRS[d][0], edge, self.h, self.mr)
        c0, cn = self.span(DIRS[d][1], edge, self.w, self.mc)
        return pl.ds(r0, rn), pl.ds(B * c0, B * cn), rn, B * cn


E1 = Halo(HC, WC, 2, 2)
E2 = Halo(HF, WF, 2, 2)
E3 = Halo(HC, WC, 4, 4)
E4 = Halo(HF, WF, 3, 4)
HALOS = (E1, E2, E3, E4)


def decoder(
    n_row,
    n_col,
    prev_hbm,
    skipc_hbm,
    skipf_hbm,
    wc_hbm,
    wf_hbm,
    bc_ref,
    bf_ref,
    proj_ref,
    offset_ref,
    permc_ref,
    permf_ref,
    upc_ref,
    out_ref,
    prev_in,
    skipc_in,
    skipf_in,
    wc,
    wf,
    s1c,
    s1f,
    s2c,
    s2f,
    pc,
    a0c,
    a4c,
    g0c,
    g4c,
    a0f,
    a4f,
    g0f,
    g4f,
    tc,
    joined,
    sb1,
    sb2,
    sb3,
    sb4,
    rb1,
    rb2,
    rb3,
    rb4,
    load_sem,
    send_sem,
    recv_sem,
):
    row = lax.axis_index("row")
    col = lax.axis_index("col")
    sends = (sb1, sb2, sb3, sb4)
    recvs = (rb1, rb2, rb3, rb4)

    def exists(d):
        dr, dc = DIRS[d]
        ok = None
        for coord, step, count in ((row, dr, n_row), (col, dc, n_col)):
            if step:
                test = (coord > 0) if step < 0 else (coord < count - 1)
                ok = test if ok is None else ok & test
        return ok

    def each(fn):
        for d in range(8):
            pl.when(exists(d))(functools.partial(fn, d))

    def peer(d):
        return (row + DIRS[d][0], col + DIRS[d][1])

    barrier = pltpu.get_barrier_semaphore()

    def greet(d):
        pl.semaphore_signal(barrier, inc=1, device_id=peer(d), device_id_type=MESH)

    each(greet)

    loads = []
    for src, dst in (
        [(skipc_hbm, skipc_in), (skipf_hbm, skipf_in), (prev_hbm, prev_in)]
        + [(wc_hbm.at[k], wc.at[k]) for k in (0, 1)]
        + [(wf_hbm.at[k], wf.at[k]) for k in (0, 1)]
        + [(wc_hbm.at[k], wc.at[k]) for k in (2, 3)]
        + [(wf_hbm.at[k], wf.at[k]) for k in (2, 3)]
    ):
        copy = pltpu.make_async_copy(src, dst, load_sem.at[len(loads)])
        copy.start()
        loads.append(copy)
    load_skipc, load_skipf, load_prev = loads[:3]
    load_c = [loads[3], loads[4], loads[7], loads[8]]
    load_f = [loads[5], loads[6], loads[9], loads[10]]

    def copy_of(e, d):
        halo = HALOS[e]
        return pltpu.make_async_remote_copy(
            src_ref=sends[e].at[halo.part(d)],
            dst_ref=recvs[e].at[halo.part(d ^ 1)],
            send_sem=send_sem.at[e, d],
            recv_sem=recv_sem.at[e, d ^ 1],
            device_id=peer(d),
            device_id_type=MESH,
        )

    def arrival_of(e, d):
        halo = HALOS[e]
        return pltpu.make_async_remote_copy(
            src_ref=sends[e].at[halo.part(d)],
            dst_ref=recvs[e].at[halo.part(d)],
            send_sem=send_sem.at[e, d],
            recv_sem=recv_sem.at[e, d],
            device_id=peer(d),
            device_id_type=MESH,
        )

    def pack(e, values):
        halo = HALOS[e]
        for d in range(8):
            rows, cols, rn, cn = halo.box(d, True)
            tile = values[rows, cols, :].reshape(rn * cn, C)
            sends[e][halo.part(d), :] = tile.astype(BF16)

    def send(e):
        each(lambda d: copy_of(e, d).start())

    def receive(e, values):
        halo = HALOS[e]

        def take(d):
            arrival_of(e, d).wait_recv()
            rows, cols, rn, cn = halo.box(d, False)
            tile = recvs[e][halo.part(d), :].astype(F32)
            values[rows, cols, :] = tile.reshape(rn, cn, C)

        each(take)

    def relayout(src, perm, height, width, dst, row0, off):
        group = 4

        def step(i, carry):
            for j in range(group):
                h = i * group + j
                flat = src[:, h].astype(F32).reshape(B * width, C).astype(BF16)
                dst[row0 + h, pl.ds(off, B * width), :] = jnp.dot(
                    perm[...], flat, preferred_element_type=F32
                )
            return carry

        lax.fori_loop(0, height // group, step, 0)

    def activate(values, shift, height, width, a0, a4, extra=None):
        n = B * width
        group = 2

        def step(i, carry):
            h = i * group
            if extra is not None:
                values[pl.ds(h, group)] = values[pl.ds(h, group)] + extra[pl.ds(h + 1, group)]
            v = jnp.maximum(values[pl.ds(h, group), pl.ds(shift, n), :], 0.0)
            a0[pl.ds(h, group), pl.ds(0, n), :] = v
            a4[pl.ds(h, group), pl.ds(B, n), :] = v
            return carry

        lax.fori_loop(0, height // group, step, 0)

    def zero_outside(a0, a4, margin, height, width):
        full = B * (width + 2 * margin)

        def wipe(r0, rn, c0, cn):
            blank = jnp.zeros((rn, cn, C), F32)
            a0[pl.ds(r0, rn), pl.ds(c0, cn), :] = blank
            a4[pl.ds(r0, rn), pl.ds(c0 + B, cn), :] = blank

        tall = height + 2 * margin
        pl.when(row == 0)(lambda: wipe(0, margin, 0, full))
        pl.when(row == n_row - 1)(lambda: wipe(margin + height, margin, 0, full))
        pl.when(col == 0)(lambda: wipe(0, tall, 0, B * margin))
        pl.when(col == n_col - 1)(lambda: wipe(0, tall, B * (margin + width), B * margin))

    def conv(a0, a4, w, k, bias, height, width, chunk, emit):
        n = B * width

        def step(i, carry):
            h = jnp.minimum(i * chunk, height - chunk)
            total = None
            for dy in range(3):
                for dx in range(3):
                    src = a4 if dx == 1 else a0
                    first = 8 if dx else 0
                    tap = src[pl.ds(h + dy, chunk), pl.ds(first, n), :]
                    part = jnp.dot(
                        tap.reshape(chunk * n, C).astype(BF16),
                        w[k, 3 * dy + dx],
                        preferred_element_type=F32,
                    )
                    total = part if total is None else total + part
            emit(h, (total + bias[pl.ds(k, 1), :]).reshape(chunk, n, C))
            return carry

        steps = -(-height // chunk)
        if steps == 1:
            step(0, 0)
        else:
            lax.fori_loop(0, steps, step, 0)

    def to_hidden(g0, g4, width, chunk):
        def emit(h, r):
            r = jnp.maximum(r, 0.0)
            g0[pl.ds(h, chunk), pl.ds(0, B * width), :] = r
            g4[pl.ds(h, chunk), pl.ds(B, B * width), :] = r

        return emit

    load_skipc.wait()
    relayout(skipc_in, permc_ref, HC, WC, s1c, E1.mr, E1.off)
    pack(0, s1c)
    load_skipf.wait()
    relayout(skipf_in, permf_ref, HF, WF, s1f, E2.mr, E2.off)
    pack(1, s1f)
    tall_peers = (row > 0).astype(jnp.int32) + (row < n_row - 1).astype(jnp.int32)
    wide_peers = (col > 0).astype(jnp.int32) + (col < n_col - 1).astype(jnp.int32)
    pl.semaphore_wait(barrier, tall_peers + wide_peers + tall_peers * wide_peers)
    send(0)
    send(1)
    load_prev.wait()
    relayout(prev_in, permc_ref, HC, WC, pc, 0, 0)

    receive(0, s1c)
    activate(s1c, 0, HC + 4, WC + 4, a0c, a4c)
    zero_outside(a0c, a4c, 2, HC, WC)
    load_c[0].wait()
    conv(a0c, a4c, wc, 0, bc_ref, HC + 2, WC + 2, HC + 2, to_hidden(g0c, g4c, WC + 2, HC + 2))
    zero_outside(g0c, g4c, 1, HC, WC)

    def emit_sum_coarse(h, r):
        own = s1c[pl.ds(E1.mr, HC), pl.ds(E1.off, B * WC), :]
        s2c[pl.ds(E3.mr, HC), pl.ds(E3.off, B * WC), :] = r + own + pc[...]

    load_c[1].wait()
    conv(g0c, g4c, wc, 1, bc_ref, HC, WC, HC, emit_sum_coarse)
    pack(2, s2c)
    send(2)

    receive(1, s1f)
    activate(s1f, 0, HF + 4, WF + 4, a0f, a4f)
    zero_outside(a0f, a4f, 2, HF, WF)
    load_f[0].wait()
    conv(a0f, a4f, wf, 0, bf_ref, HF + 2, WF + 2, 12, to_hidden(g0f, g4f, WF + 2, 12))
    zero_outside(g0f, g4f, 1, HF, WF)

    def emit_unit_fine(h, r):
        own = s1f[pl.ds(h + E2.mr, 16), pl.ds(E2.off, B * WF), :]
        s2f[pl.ds(h + E4.mr, 16), pl.ds(E4.off, B * WF), :] = r + own

    load_f[1].wait()
    conv(g0f, g4f, wf, 1, bf_ref, HF, WF, 16, emit_unit_fine)
    pack(3, s2f)
    send(3)

    receive(2, s2c)
    activate(s2c, 0, HC + 8, WC + 8, a0c, a4c)
    zero_outside(a0c, a4c, 4, HC, WC)
    load_c[2].wait()
    conv(a0c, a4c, wc, 2, bc_ref, HC + 6, WC + 6, HC + 6, to_hidden(g0c, g4c, WC + 6, HC + 6))
    zero_outside(g0c, g4c, 3, HC, WC)
    tall, wide = HC + 4, B * (WC + 4)

    def emit_top_coarse(h, r):
        tc[pl.ds(1, tall), :, :] = (r + s2c[pl.ds(2, tall), pl.ds(8, wide), :]).astype(BF16)

    load_c[3].wait()
    conv(g0c, g4c, wc, 3, bc_ref, HC + 4, WC + 4, HC + 4, emit_top_coarse)

    tc[0] = jnp.zeros((wide, C), BF16)
    tc[tall + 1] = jnp.zeros((wide, C), BF16)

    def repeat_rows(buf, dst, src):
        for r in dst:
            buf[r] = buf[src]

    def repeat_cols(buf, height, width, dst, src):
        def step(h, carry):
            v = buf[h].astype(F32)
            parts = [v[B * j : B * j + B] for j in range(width)]
            for j in dst:
                parts[j] = parts[src]
            buf[h] = jnp.concatenate(parts + [v[B * width :]] if v.shape[0] > B * width else parts, axis=0).astype(BF16)
            return carry

        lax.fori_loop(0, height, step, 0)

    pl.when(row == 0)(lambda: repeat_rows(tc, (1, 2), 3))
    pl.when(row == n_row - 1)(lambda: repeat_rows(tc, (HC + 3, HC + 4), HC + 2))
    pl.when(col == 0)(lambda: repeat_cols(tc, HC + 6, WC + 4, (0, 1), 2))
    pl.when(col == n_col - 1)(lambda: repeat_cols(tc, HC + 6, WC + 4, (WC + 2, WC + 3), WC + 1))

    def join(i, carry):
        for j in range(2):
            k = 2 * i + j
            near = tc[pl.ds(k, 3)].reshape(3 * wide, C)
            up = jnp.dot(upc_ref[...], near, preferred_element_type=F32).astype(BF16)
            r = jnp.dot(up, proj_ref[...], preferred_element_type=F32) + offset_ref[...]
            joined[pl.ds(2 * k, 2)] = r.astype(BF16).astype(F32).reshape(2, 2 * wide, C)
        return carry

    lax.fori_loop(0, tall // 2, join, 0)

    receive(3, s2f)
    activate(s2f, B, HF + 6, WF + 6, a0f, a4f, joined)
    zero_outside(a0f, a4f, 3, HF, WF)
    load_f[2].wait()
    conv(a0f, a4f, wf, 2, bf_ref, HF + 4, WF + 4, 12, to_hidden(g0f, g4f, WF + 4, 12))
    zero_outside(g0f, g4f, 2, HF, WF)
    n = B * (WF + 2)

    def emit_top_fine(h, r):
        own = s2f[pl.ds(h + 2, 12), pl.ds(3 * B, n), :]
        pad = jnp.zeros((12, 8, C), F32)
        out_ref[pl.ds(h, 12)] = jnp.concatenate([r + own, pad], axis=1).astype(BF16)

    load_f[3].wait()
    conv(g0f, g4f, wf, 3, bf_ref, HF + 2, WF + 2, 12, emit_top_fine)
    pl.when(row == 0)(lambda: repeat_rows(out_ref, (0,), 1))
    pl.when(row == n_row - 1)(lambda: repeat_rows(out_ref, (HF + 1,), HF))
    pl.when(col == 0)(lambda: repeat_cols(out_ref, HF + 2, WF + 2, (0,), 1))
    pl.when(col == n_col - 1)(lambda: repeat_cols(out_ref, HF + 2, WF + 2, (WF + 1,), WF))

    for e in range(4):
        each(lambda d, e=e: copy_of(e, d).wait_send())


def finish(top_ref, up_ref, proj_ref, offset_ref, out_ref):
    start = pl.program_id(0) * 4
    for j in range(4):
        near = top_ref[pl.ds(start + j, 3)].reshape(3 * B * (WF + 4), C)
        up = jnp.dot(up_ref[...], near, preferred_element_type=F32).astype(BF16)
        r = jnp.dot(up, proj_ref[...], preferred_element_type=F32) + offset_ref[...]
        r = r.astype(BF16).reshape(2, B, 2 * WF, C)
        out_ref[:, 2 * j] = r[0]
        out_ref[:, 2 * j + 1] = r[1]


def interleave(width):
    m = np.zeros((B * width, B * width), np.float32)
    for w in range(width):
        for b in range(B):
            m[w * B + b, b * width + w] = 1.0
    return m


def doubling(cols, out_cols, pitch, place, first):
    m = np.zeros((2 * B * out_cols, 3 * pitch), np.float32)
    for parity in range(2):
        for f in range(out_cols):
            c = first + f // 2
            beside = min(max(c + (1 if f % 2 else -1), 0), cols - 1)
            for b in range(B):
                out = parity * B * out_cols + place(f, b)
                for r, wr in ((1, 0.75), (2 if parity else 0, 0.25)):
                    m[out, r * pitch + c * B + b] += 0.75 * wr
                    m[out, r * pitch + beside * B + b] += 0.25 * wr
    return m


def per_device(n_row, n_col, previous, skip_coarse, skip_fine, coarse_convs, coarse_biases, coarse_project,
               coarse_offset, fine_convs, fine_biases, fine_project, fine_offset):
    wc = coarse_convs.reshape(4, 9, C, C)
    wf = fine_convs.reshape(4, 9, C, C)
    permc = jnp.asarray(interleave(WC), BF16)
    permf = jnp.asarray(interleave(WF), BF16)
    upc = jnp.asarray(doubling(WC + 4, 2 * (WC + 4), B * (WC + 4), lambda f, b: f * B + b, 0), BF16)
    upf = jnp.asarray(doubling(WF + 2, 2 * WF, B * (WF + 4), lambda f, b: b * 2 * WF + f, 1), BF16)
    vmem = pl.BlockSpec(memory_space=pltpu.VMEM)
    anywhere = pl.BlockSpec(memory_space=pl.ANY)

    def block(rows, subs, dtype=F32):
        return pltpu.VMEM((rows, subs, C), dtype)

    top = pl.pallas_call(
        functools.partial(decoder, n_row, n_col),
        out_shape=jax.ShapeDtypeStruct((HF + 2, B * (WF + 4), C), BF16),
        in_specs=[anywhere] * 5 + [vmem] * 7,
        out_specs=vmem,
        scratch_shapes=[
            pltpu.VMEM((B, HC, WC, C), BF16),
            pltpu.VMEM((B, HC, WC, C), BF16),
            pltpu.VMEM((B, HF, WF, C), BF16),
            pltpu.VMEM((4, 9, C, C), BF16),
            pltpu.VMEM((4, 9, C, C), BF16),
            block(HC + 4, B * (WC + 4)),
            block(HF + 4, B * (WF + 4)),
            block(HC + 8, B * (WC + 8)),
            block(HF + 6, B * (WF + 8)),
            block(HC, B * WC),
            block(HC + 8, B * (WC + 8)),
            block(HC + 8, B * (WC + 8) + 8),
            block(HC + 6, B * (WC + 6)),
            block(HC + 6, B * (WC + 6) + 8),
            block(HF + 6, B * (WF + 6)),
            block(HF + 6, B * (WF + 6) + 8),
            block(HF + 4, B * (WF + 4)),
            block(HF + 4, B * (WF + 4) + 8),
            block(HC + 6, B * (WC + 4), BF16),
            block(2 * (HC + 4), 2 * B * (WC + 4)),
        ]
        + [pltpu.VMEM((halo.total, C), BF16) for halo in HALOS] * 2
        + [
            pltpu.SemaphoreType.DMA((11,)),
            pltpu.SemaphoreType.DMA((4, 8)),
            pltpu.SemaphoreType.DMA((4, 8)),
        ],
        compiler_params=pltpu.CompilerParams(
            collective_id=0, has_side_effects=True, vmem_limit_bytes=62 * 2**20
        ),
        name="decoder",
    )(
        previous,
        skip_coarse,
        skip_fine,
        wc,
        wf,
        coarse_biases,
        fine_biases,
        coarse_project,
        coarse_offset.reshape(1, C),
        permc,
        permf,
        upc,
    )
    return pl.pallas_call(
        finish,
        grid=(HF // 4,),
        out_shape=jax.ShapeDtypeStruct((B, 2 * HF, 2 * WF, C), BF16),
        in_specs=[vmem] * 4,
        out_specs=pl.BlockSpec((B, 8, 2 * WF, C), lambda i: (0, i, 0, 0)),
        compiler_params=pltpu.CompilerParams(vmem_limit_bytes=32 * 2**20),
        name="finish",
    )(top, upf, fine_project, fine_offset.reshape(1, C))


def solution(mesh):
    tiled = P(None, "row", "col", None)
    return jax.shard_map(
        functools.partial(per_device, mesh.shape["row"], mesh.shape["col"]),
        mesh=mesh,
        in_specs=(tiled,) * 3 + (P(),) * 8,
        out_specs=tiled,
        check_vma=False,
    )
```
